16 devices in a mesh: fsdp: 16 (over z, y, x, core).
Axes of the slice: x: 2, y: 2, z: 2, core: 2. Of those that a mesh axis runs over, the one named last changes fastest.
Arguments:
- timesteps: float32 [8192], P('fsdp')
- guidance: float32 [8192], P('fsdp')
- pooled: bfloat16 [8192, 2048], P('fsdp')
- time_w1: bfloat16 [256, 1536], replicated
- time_b1: bfloat16 [1536], replicated
- time_w2: bfloat16 [1536, 1536], replicated
- time_b2: bfloat16 [1536], replicated
- guide_w1: bfloat16 [256, 1536], replicated
- guide_b1: bfloat16 [1536], replicated
- guide_w2: bfloat16 [1536, 1536], replicated
- guide_b2: bfloat16 [1536], replicated
- text_w1: bfloat16 [2048, 1536], replicated
- text_b1: bfloat16 [1536], replicated
- text_w2: bfloat16 [1536, 1536], replicated
- text_b2: bfloat16 [1536], replicated
- w_mod: bfloat16 [1536, 30720], P(None, 'fsdp')
- b_mod: bfloat16 [30720], P('fsdp')
- d_mods: bfloat16 [8192, 30720], P('fsdp')
Outputs:
- output 1: bfloat16 [8192, 30720], P('fsdp')
- output 2: float32 [1536, 30720], P(None, 'fsdp')
- output 3: float32 [30720], P('fsdp')
- output 4: float32 [256, 1536], replicated
- output 5: float32 [1536], replicated
- output 6: float32 [1536, 1536], replicated
- output 7: float32 [1536], replicated
- output 8: float32 [256, 1536], replicated
- output 9: float32 [1536], replicated
- output 10: float32 [1536, 1536], replicated
- output 11: float32 [1536], replicated
- output 12: float32 [2048, 1536], replicated
- output 13: float32 [1536], replicated
- output 14: float32 [1536, 1536], replicated
- output 15: float32 [1536], replicated
All inputs are finite; a program needn't handle non-finite values.
Results may differ from the reference program's by a relative error of at most 0.00492024.
Values are sent between devices in bfloat16 or wider.
A program may use at most 1 GiB of HBM per device.

```python
import math
import jax
import jax.numpy as jnp

GLOBAL_BATCH = 8192
HIDDEN = 1536
POOL_WIDTH = 2048
FREQ_WIDTH = 256
MOD_WIDTH = 30720


def setup_inputs(seed: int = 0) -> dict:
    key_list = jax.random.split(jax.random.key(seed), 18)

    def draw_weight(sub_key, fan_in, fan_out):
        return (jax.random.normal(sub_key, (fan_in, fan_out), jnp.float32) * fan_in ** -0.5).astype(jnp.bfloat16)

    def draw_bias(sub_key, fan_out):
        return (0.5 * jax.random.normal(sub_key, (fan_out,), jnp.float32)).astype(jnp.bfloat16)

    grad_scale = GLOBAL_BATCH ** -0.5
    return dict(
        timesteps=jax.random.uniform(key_list[0], (GLOBAL_BATCH,), jnp.float32),
        guidance=jax.random.uniform(key_list[1], (GLOBAL_BATCH,), jnp.float32, 1.0, 5.0),
        pooled=jax.random.normal(key_list[2], (GLOBAL_BATCH, POOL_WIDTH), jnp.float32).astype(jnp.bfloat16),
        time_w1=draw_weight(key_list[3], FREQ_WIDTH, HIDDEN),
        time_b1=draw_bias(key_list[4], HIDDEN),
        time_w2=draw_weight(key_list[5], HIDDEN, HIDDEN),
        time_b2=draw_bias(key_list[6], HIDDEN),
        guide_w1=draw_weight(key_list[7], FREQ_WIDTH, HIDDEN),
        guide_b1=draw_bias(key_list[8], HIDDEN),
        guide_w2=draw_weight(key_list[9], HIDDEN, HIDDEN),
        guide_b2=draw_bias(key_list[10], HIDDEN),
        text_w1=draw_weight(key_list[11], POOL_WIDTH, HIDDEN),
        text_b1=draw_bias(key_list[12], HIDDEN),
        text_w2=draw_weight(key_list[13], HIDDEN, HIDDEN),
        text_b2=draw_bias(key_list[14], HIDDEN),
        w_mod=draw_weight(key_list[15], HIDDEN, MOD_WIDTH),
        b_mod=draw_bias(key_list[16], MOD_WIDTH),
        d_mods=(jax.random.normal(key_list[17], (GLOBAL_BATCH, MOD_WIDTH), jnp.float32) * grad_scale).astype(jnp.bfloat16),
    )


def sinusoid(values):
    half_width = FREQ_WIDTH // 2
    freq_table = jnp.exp(-math.log(10000.0) * jnp.arange(half_width, dtype=jnp.float32) / half_width)
    angles = (1000.0 * values)[:, None] * freq_table[None, :]
    return jnp.concatenate([jnp.cos(angles), jnp.sin(angles)], axis=1).astype(jnp.bfloat16)


def silu_grad(values):
    sigmoid_v = jax.nn.sigmoid(values)
    return sigmoid_v * (1.0 + values * (1.0 - sigmoid_v))


def mlp_forward(inputs_bf, params):
    hidden = jnp.dot(inputs_bf, params[0], preferred_element_type=jnp.float32) + params[1].astype(jnp.float32)
    act_bf = jax.nn.silu(hidden).astype(jnp.bfloat16)
    output = jnp.dot(act_bf, params[2], preferred_element_type=jnp.float32) + params[3].astype(jnp.float32)
    return output, hidden, act_bf


def mlp_backward(inputs_bf, params, hidden, act_bf, d_out, d_out_bf):
    grad_w2 = jnp.dot(act_bf.T, d_out_bf, preferred_element_type=jnp.float32)
    grad_b2 = jnp.sum(d_out, axis=0)
    d_act = jnp.dot(d_out_bf, params[2].T, preferred_element_type=jnp.float32)
    d_hidden = d_act * silu_grad(hidden)
    grad_w1 = jnp.dot(inputs_bf.T, d_hidden.astype(jnp.bfloat16), preferred_element_type=jnp.float32)
    grad_b1 = jnp.sum(d_hidden, axis=0)
    return grad_w1, grad_b1, grad_w2, grad_b2


def reference(timesteps, guidance, pooled, time_w1, time_b1, time_w2, time_b2, guide_w1, guide_b1, guide_w2, guide_b2, text_w1, text_b1, text_w2, text_b2, w_mod, b_mod, d_mods):
    inputs_list = [sinusoid(timesteps), sinusoid(guidance), pooled]
    params_list = [(time_w1, time_b1, time_w2, time_b2), (guide_w1, guide_b1, guide_w2, guide_b2), (text_w1, text_b1, text_w2, text_b2)]
    saved_acts = [mlp_forward(inputs_bf, params) for inputs_bf, params in zip(inputs_list, params_list)]
    cond_vec = saved_acts[0][0] + saved_acts[1][0] + saved_acts[2][0]
    cond_silu = jax.nn.silu(cond_vec).astype(jnp.bfloat16)
    modulation = (jnp.dot(cond_silu, w_mod, preferred_element_type=jnp.float32) + b_mod.astype(jnp.float32)).astype(jnp.bfloat16)
    grad_wmod = jnp.dot(cond_silu.T, d_mods, preferred_element_type=jnp.float32)
    grad_bmod = jnp.sum(d_mods, axis=0, dtype=jnp.float32)
    d_cond = jnp.dot(d_mods, w_mod.T, preferred_element_type=jnp.float32)
    d_vec = d_cond * silu_grad(cond_vec)
    d_vec_bf = d_vec.astype(jnp.bfloat16)
    time_grads = mlp_backward(inputs_list[0], params_list[0], saved_acts[0][1], saved_acts[0][2], d_vec, d_vec_bf)
    guide_grads = mlp_backward(inputs_list[1], params_list[1], saved_acts[1][1], saved_acts[1][2], d_vec, d_vec_bf)
    text_grads = mlp_backward(inputs_list[2], params_list[2], saved_acts[2][1], saved_acts[2][2], d_vec, d_vec_bf)
    return (modulation, grad_wmod, grad_bmod, time_grads[0], time_grads[1], time_grads[2], time_grads[3], guide_grads[0], guide_grads[1], guide_grads[2], guide_grads[3], text_grads[0], text_grads[1], text_grads[2], text_grads[3])
```

```python
import math
import jax
import jax.numpy as jnp
from jax import lax
from jax.experimental import pallas as pl
from jax.experimental.pallas import tpu as pltpu
from jax.sharding import PartitionSpec as P

MESH_AXIS = "fsdp"
MAX_PERIOD = 10000.0
TIME_SCALE = 1000.0
CONTRACT_ROWS = (((0,), (0,)), ((), ()))
CONTRACT_COLS = (((1,), (1,)), ((), ()))
COLOURS = ((2, 4, 8), (4, 8, 2), (8, 2, 4))
G_GROUPS = ((2, 3, 4, 5, 8, 9), (6, 7, 10, 11, 12, 13), (14, 15))
CALLS = ((0, 1), (2, 3), (4, 5), (6,), (7,))
ROUNDS = (((), 0), ((), 1), ((), 2), ((0,), 1), ((0,), 2), ((1,), 2), ((0, 1), 2))
VMEM_LIMIT = 60 * 1024 * 1024


def sinusoid(values, freq_width):
    half_width = freq_width // 2
    freq_table = jnp.exp(-math.log(MAX_PERIOD) * jnp.arange(half_width, dtype=jnp.float32) / half_width)
    angles = (TIME_SCALE * values)[:, None] * freq_table[None, :]
    return jnp.concatenate([jnp.cos(angles), jnp.sin(angles)], axis=1).astype(jnp.bfloat16)


def silu_grad(values):
    sigmoid_v = jax.nn.sigmoid(values)
    return sigmoid_v * (1.0 + values * (1.0 - sigmoid_v))


def mlp_forward(inputs_bf, params):
    hidden = jnp.dot(inputs_bf, params[0], preferred_element_type=jnp.float32) + params[1].astype(jnp.float32)
    act_bf = jax.nn.silu(hidden).astype(jnp.bfloat16)
    return jnp.dot(act_bf, params[2], preferred_element_type=jnp.float32) + params[3].astype(jnp.float32)


def cost(flops, bytes_accessed):
    return pl.CostEstimate(flops=flops, bytes_accessed=bytes_accessed, transcendentals=0)


def dot_f32(a, b, dims):
    return lax.dot_general(a, b, dims, preferred_element_type=jnp.float32)


def split_for_partner(core, d_mods, n_dev, cols):
    rows = d_mods.shape[0]

    def body(core_ref, src_ref, dst_ref):
        dst_ref[0] = src_ref[...]

    return pl.pallas_call(
        body,
        name="split_for_partner",
        grid_spec=pltpu.PrefetchScalarGridSpec(
            num_scalar_prefetch=1,
            grid=(n_dev // 2,),
            in_specs=[pl.BlockSpec((rows, cols), lambda j, c: (0, 2 * j + 1 - c[0]))],
            out_specs=pl.BlockSpec((1, rows, cols), lambda j, c: (j, 0, 0)),
        ),
        out_shape=jax.ShapeDtypeStruct((n_dev // 2, rows, cols), d_mods.dtype),
        cost_estimate=cost(n_dev * rows * cols, 2 * n_dev * rows * cols),
    )(core, d_mods)


def place_blocks(core, modulation, blocks):
    chips, rows, cols = blocks.shape

    def body(core_ref, src_ref, old_ref, dst_ref):
        dst_ref[...] = src_ref[0]

    return pl.pallas_call(
        body,
        name="place_blocks",
        grid_spec=pltpu.PrefetchScalarGridSpec(
            num_scalar_prefetch=1,
            grid=(chips,),
            in_specs=[pl.BlockSpec((1, rows, cols), lambda j, c: (j, 0, 0)), pl.BlockSpec(memory_space=pl.ANY)],
            out_specs=pl.BlockSpec((rows, cols), lambda j, c: (0, 2 * j + 1 - c[0])),
        ),
        out_shape=jax.ShapeDtypeStruct(modulation.shape, modulation.dtype),
        input_output_aliases={2: 0},
        cost_estimate=cost(2 * chips * rows * cols, 4 * chips * rows * cols),
    )(core, blocks, modulation)


def column_rounds(where, s_own, s_their, g_own, g_their, bias, w_blocks, carry):
    n = len(w_blocks)
    hidden, width = w_blocks[0].shape
    rows = s_own.shape[0]
    chips, _, cols = g_their.shape
    total = g_own.shape[1]
    first = carry is None

    def body(where_ref, so_ref, st_ref, go_ref, gt_ref, b_ref, *refs):
        w_refs, refs = refs[:n], refs[n:]
        if not first:
            old_ref, refs = refs[0], refs[3:]
        mo_ref, mt_ref, dc_ref = refs
        step = pl.program_id(0)

        @pl.when(step == 0)
        def _():
            dc_ref[...] = jnp.zeros_like(dc_ref) if first else old_ref[...]

        for k in range(n):
            @pl.when(step == k)
            def _(k=k):
                w = w_refs[k][...]
                dc_ref[:rows] += dot_f32(go_ref[...], w, CONTRACT_COLS)
                dc_ref[rows:] += dot_f32(gt_ref[0], w, CONTRACT_COLS)
                mo_ref[...] = (jnp.dot(so_ref[...], w, preferred_element_type=jnp.float32) + b_ref[...]).astype(mo_ref.dtype)
                mt_ref[0] = (jnp.dot(st_ref[...], w, preferred_element_type=jnp.float32) + b_ref[...]).astype(mt_ref.dtype)

    def own_col(k, w):
        return 0, w[k]

    def their_col(k, w):
        return w[n + k], 0, w[2 * n + k]

    fixed = lambda k, w: (0, 0)
    once = pl.Buffered(1)
    in_specs = [pl.BlockSpec((rows, hidden), fixed, pipeline_mode=once)] * 2
    in_specs += [pl.BlockSpec((rows, width), own_col), pl.BlockSpec((1, rows, width), their_col), pl.BlockSpec((1, width), own_col)]
    in_specs += [pl.BlockSpec((hidden, width), fixed, pipeline_mode=once)] * n
    operands = [s_own, s_their, g_own, g_their, bias, *w_blocks]
    aliases = {}
    if not first:
        in_specs += [pl.BlockSpec((2 * rows, hidden), fixed, pipeline_mode=once), pl.BlockSpec(memory_space=pl.ANY), pl.BlockSpec(memory_space=pl.ANY)]
        operands += [carry[2], carry[0], carry[1]]
        base = 1 + 5 + n
        aliases = {base: 2, base + 1: 0, base + 2: 1}
    return pl.pallas_call(
        body,
        name="column_rounds",
        grid_spec=pltpu.PrefetchScalarGridSpec(
            num_scalar_prefetch=1,
            grid=(n,),
            in_specs=in_specs,
            out_specs=[pl.BlockSpec((rows, width), own_col), pl.BlockSpec((1, rows, width), their_col), pl.BlockSpec((2 * rows, hidden), fixed)],
        ),
        out_shape=[jax.ShapeDtypeStruct((rows, total), jnp.bfloat16), jax.ShapeDtypeStruct((chips, rows, cols), jnp.bfloat16), jax.ShapeDtypeStruct((2 * rows, hidden), jnp.float32)],
        input_output_aliases=aliases,
        cost_estimate=cost(8 * n * rows * hidden * width, 2 * n * hidden * width + 8 * n * rows * width),
        compiler_params=pltpu.CompilerParams(vmem_limit_bytes=VMEM_LIMIT),
    )(where, *operands)


def sum_silu(core, part_cond, incoming, bias):
    batch, hidden = part_cond.shape
    block = 512
    steps = batch // 2 // block

    def body(core_ref, a_ref, b_ref, bias_ref, out_ref):
        value = a_ref[...] + b_ref[...] + bias_ref[...]
        out_ref[...] = (value * jax.nn.sigmoid(value)).astype(jnp.bfloat16).T

    return pl.pallas_call(
        body,
        name="sum_silu",
        grid_spec=pltpu.PrefetchScalarGridSpec(
            num_scalar_prefetch=1,
            grid=(steps,),
            in_specs=[pl.BlockSpec((block, hidden), lambda i, c: (i + c[0] * steps, 0)), pl.BlockSpec((block, hidden), lambda i, c: (i, 0)), pl.BlockSpec((1, hidden), lambda i, c: (0, 0))],
            out_specs=pl.BlockSpec((hidden, block), lambda i, c: (0, i)),
        ),
        out_shape=jax.ShapeDtypeStruct((hidden, batch // 2), jnp.bfloat16),
        cost_estimate=cost(4 * batch * hidden, 10 * batch // 2 * hidden),
        compiler_params=pltpu.CompilerParams(vmem_limit_bytes=VMEM_LIMIT),
    )(core, part_cond, incoming, bias)


def embed_body(core_ref, t_ref, g_ref, u_ref, wt1, wg1, wu1, bt1, bg1, bu1, wt2, wg2, wu2, h_ref, c_ref):
    total = None
    for k, (x_ref, w1, b1, w2) in enumerate(((t_ref, wt1, bt1, wt2), (g_ref, wg1, bg1, wg2), (u_ref, wu1, bu1, wu2))):
        hidden = jnp.dot(x_ref[...], w1[...], preferred_element_type=jnp.float32) + b1[...]
        h_ref[k] = hidden
        act = (hidden * jax.nn.sigmoid(hidden)).astype(jnp.bfloat16)
        part = jnp.dot(act, w2[...], preferred_element_type=jnp.float32)
        total = part if total is None else total + part
    c_ref[...] = total


def embed_half(core, inputs_list, params_list, block):
    batch = inputs_list[0].shape[0]
    hidden, out_width = params_list[0][2].shape
    half = hidden // 2
    rows = [pl.BlockSpec((block, x.shape[1]), lambda i, c: (i, 0)) for x in inputs_list]
    firsts = [pl.BlockSpec((p[0].shape[0], half), lambda i, c: (0, c[0])) for p in params_list]
    biases = [pl.BlockSpec((1, half), lambda i, c: (0, c[0])) for p in params_list]
    seconds = [pl.BlockSpec((half, out_width), lambda i, c: (c[0], 0)) for p in params_list]
    flops = sum(2 * batch * half * (p[0].shape[0] + out_width) for p in params_list)
    return pl.pallas_call(
        embed_body,
        name="embed_half",
        grid_spec=pltpu.PrefetchScalarGridSpec(
            num_scalar_prefetch=1,
            grid=(batch // block,),
            in_specs=rows + firsts + biases + seconds,
            out_specs=[pl.BlockSpec((3, block, half), lambda i, c: (0, i, 0)), pl.BlockSpec((block, out_width), lambda i, c: (i, 0))],
        ),
        out_shape=[jax.ShapeDtypeStruct((3, batch, half), jnp.float32), jax.ShapeDtypeStruct((batch, out_width), jnp.float32)],
        cost_estimate=cost(flops, 4 * batch * (3 * half + out_width)),
        compiler_params=pltpu.CompilerParams(vmem_limit_bytes=VMEM_LIMIT),
    )(core, *inputs_list, *(p[0] for p in params_list), *(p[1].astype(jnp.float32)[None] for p in params_list), *(p[2] for p in params_list))


def embed_grad_body(n_mlp, *refs):
    d_ref, refs = refs[0], refs[1:]
    x_refs, h_refs, w2_refs, outs = refs[:n_mlp], refs[n_mlp:2 * n_mlp], refs[2 * n_mlp:3 * n_mlp], refs[3 * n_mlp:]

    @pl.when(pl.program_id(0) == 0)
    def _():
        for out in outs:
            out[...] = jnp.zeros_like(out)

    for k in range(n_mlp):
        g1_ref, b1_ref, g2_ref = outs[3 * k:3 * k + 3]
        hidden = h_refs[k][0]
        sig = jax.nn.sigmoid(hidden)
        act = (hidden * sig).astype(jnp.bfloat16)
        d_act = dot_f32(d_ref[...], w2_refs[k][...], CONTRACT_COLS)
        d_hidden = d_act * (sig * (1.0 + hidden * (1.0 - sig)))
        b1_ref[...] += jnp.sum(d_hidden, axis=0, keepdims=True)
        g2_ref[...] += dot_f32(act, d_ref[...], CONTRACT_ROWS)
        g1_ref[...] += dot_f32(x_refs[k][...], d_hidden.astype(jnp.bfloat16), CONTRACT_ROWS)


def embed_grad(core, d_vec_all, which, inputs_list, hidden_all, params_list, block):
    batch, out_width = d_vec_all.shape
    half = hidden_all.shape[2]
    n_mlp = len(which)

    def body(core_ref, *refs):
        embed_grad_body(n_mlp, *refs)

    in_specs = [pl.BlockSpec((block, out_width), lambda i, c: (i, 0))]
    in_specs += [pl.BlockSpec((block, inputs_list[k].shape[1]), lambda i, c: (i, 0)) for k in which]
    in_specs += [pl.BlockSpec((1, block, half), lambda i, c, k=k: (k, i, 0)) for k in which]
    in_specs += [pl.BlockSpec((half, out_width), lambda i, c: (c[0], 0)) for k in which]
    shapes = [s for k in which for s in ((inputs_list[k].shape[1], half), (1, half), (half, out_width))]
    flops = sum(2 * batch * half * (2 * out_width + inputs_list[k].shape[1]) for k in which)
    return pl.pallas_call(
        body,
        name="embed_grad",
        grid_spec=pltpu.PrefetchScalarGridSpec(
            num_scalar_prefetch=1,
            grid=(batch // block,),
            in_specs=in_specs,
            out_specs=[pl.BlockSpec(s, lambda i, c: (0, 0)) for s in shapes],
        ),
        out_shape=[jax.ShapeDtypeStruct(s, jnp.float32) for s in shapes],
        cost_estimate=cost(flops, 2 * batch * (out_width + 4 * half)),
        compiler_params=pltpu.CompilerParams(vmem_limit_bytes=VMEM_LIMIT),
    )(core, d_vec_all, *(inputs_list[k] for k in which), *([hidden_all] * n_mlp), *(params_list[k][2] for k in which))


def mod_weight_grad(where, mine_t, theirs_t, blocks, width, carry):
    n = len(blocks)
    hidden = mine_t.shape[0]
    rows = blocks[0][0].shape[0]
    cols = width
    tile = cols // 3
    first = carry is None

    def body(where_ref, mine_ref, theirs_ref, *refs):
        g_refs, refs = refs[:n], refs[n:]
        if not first:
            old_w, old_b, refs = refs[0], refs[1], refs[2:]
        w_ref, b_ref = refs
        step = pl.program_id(1)

        @pl.when(step == 0)
        def _():
            w_ref[...] = jnp.zeros_like(w_ref) if first else old_w[...]
            b_ref[...] = jnp.zeros_like(b_ref) if first else old_b[...]

        for k in range(n):
            @pl.when(step == k)
            def _(k=k):
                block = g_refs[k][...]
                b_ref[...] += jnp.sum(block.astype(jnp.float32), axis=0, keepdims=True)

                @pl.when(where_ref[n + k] == 1)
                def _():
                    w_ref[...] += jnp.dot(mine_ref[...], block, preferred_element_type=jnp.float32)

                @pl.when(where_ref[n + k] == 0)
                def _():
                    w_ref[...] += jnp.dot(theirs_ref[...], block, preferred_element_type=jnp.float32)

    def mine_map(t, k, w):
        return 0, jnp.where(w[n + k] == 1, w[k], 0)

    def theirs_map(t, k, w):
        return 0, jnp.where(w[n + k] == 1, 0, w[k])

    in_specs = [pl.BlockSpec((hidden, rows), mine_map), pl.BlockSpec((hidden, rows), theirs_map)]
    operands = [mine_t, theirs_t]
    for array, own in blocks:
        in_specs.append(pl.BlockSpec((rows, tile), (lambda t, k, w: (0, 3 * w[2 * n] + t)) if own else (lambda t, k, w: (0, t))))
        operands.append(array)
    out_specs = [pl.BlockSpec((hidden, tile), lambda t, k, w: (0, t)), pl.BlockSpec((1, tile), lambda t, k, w: (0, t))]
    aliases = {}
    if not first:
        in_specs += out_specs
        operands += list(carry)
        aliases = {3 + n: 0, 4 + n: 1}
    return pl.pallas_call(
        body,
        name="mod_weight_grad",
        grid_spec=pltpu.PrefetchScalarGridSpec(num_scalar_prefetch=1, grid=(3, n), in_specs=in_specs, out_specs=out_specs),
        out_shape=[jax.ShapeDtypeStruct((hidden, cols), jnp.float32), jax.ShapeDtypeStruct((1, cols), jnp.float32)],
        input_output_aliases=aliases,
        cost_estimate=cost(2 * n * rows * hidden * cols, 2 * n * rows * (3 * hidden + cols) + 8 * hidden * cols),
        compiler_params=pltpu.CompilerParams(vmem_limit_bytes=VMEM_LIMIT),
    )(where, *operands)


def join_halves(core, mine, theirs, axis):
    shape = list(mine.shape)
    shape[axis] *= 2
    block = mine.shape

    def body(core_ref, mine_ref, theirs_ref, out_ref):
        is_mine = pl.program_id(0) == core_ref[0]

        @pl.when(is_mine)
        def _():
            out_ref[...] = mine_ref[...]

        @pl.when(jnp.logical_not(is_mine))
        def _():
            out_ref[...] = theirs_ref[...]

    steps = 4 if block[1 - axis] % 32 == 0 else 1
    if axis == 0:
        part = (block[0], block[1] // steps)
        whole_map = lambda h, i, c: (h, i)
        part_map = lambda h, i, c: (0, i)
    else:
        part = (block[0] // steps, block[1])
        whole_map = lambda h, i, c: (i, h)
        part_map = lambda h, i, c: (i, 0)
    size = shape[0] * shape[1]
    return pl.pallas_call(
        body,
        name="join_halves",
        grid_spec=pltpu.PrefetchScalarGridSpec(
            num_scalar_prefetch=1,
            grid=(2, steps),
            in_specs=[pl.BlockSpec(part, part_map)] * 2,
            out_specs=pl.BlockSpec(part, whole_map),
        ),
        out_shape=jax.ShapeDtypeStruct(shape, jnp.float32),
        cost_estimate=cost(4 * size, 8 * size),
    )(core, mine, theirs)


def solution(mesh):
    n_dev = mesh.shape[MESH_AXIS]
    row_split = P(MESH_AXIS)
    row_matrix = P(MESH_AXIS, None)
    col_matrix = P(None, MESH_AXIS)
    embed_specs = (P(None, None), P(None), P(None, None), P(None)) * 3
    in_specs = (row_split, row_split, row_matrix) + embed_specs + (col_matrix, row_split, row_matrix)
    out_specs = (row_matrix, col_matrix, row_split) + embed_specs

    def send(value, bit):
        return lax.ppermute(value, MESH_AXIS, [(i, i ^ bit) for i in range(n_dev)])

    def swap(value):
        return send(value, 1)

    def local_step(timesteps, guidance, pooled, time_w1, time_b1, time_w2, time_b2, guide_w1, guide_b1, guide_w2, guide_b2, text_w1, text_b1, text_w2, text_b2, w_mod, b_mod, d_mods):
        rows, cols = d_mods.shape[0], w_mod.shape[1]
        hidden = w_mod.shape[0]
        batch = rows * n_dev
        freq_width = time_w1.shape[0]
        params_list = [(time_w1, time_b1, time_w2, time_b2), (guide_w1, guide_b1, guide_w2, guide_b2), (text_w1, text_b1, text_w2, text_b2)]
        me = lax.axis_index(MESH_AXIS)
        core_id = lax.rem(me, 2)
        chip_id = me // 2
        core = core_id.reshape(1)

        small = jnp.concatenate([timesteps, guidance, b_mod.astype(jnp.float32)])
        small_all = lax.all_gather(small, MESH_AXIS, axis=0)
        times_all = small_all[:, :rows].reshape(-1)
        guides_all = small_all[:, rows:2 * rows].reshape(-1)
        full_bmod = small_all[:, 2 * rows:].reshape(1, -1)
        pooled_all = lax.all_gather(pooled, MESH_AXIS, axis=0, tiled=True)
        g_out = split_for_partner(core, d_mods, n_dev, cols)
        g_their = swap(g_out)

        width = cols // len(COLOURS)
        held = [{0: w_mod[:, c * width:(c + 1) * width]} for c in range(len(COLOURS))]
        for source, role in ROUNDS:
            for c, bits in enumerate(COLOURS):
                have = sum(bits[i] for i in source)
                held[c][have + bits[role]] = send(held[c][have], bits[role])

        def slices(group):
            return [lax.dynamic_slice_in_dim(d_mods, jnp.bitwise_xor(me, d) * cols, cols, axis=1) for d in group]

        g_parts = {}

        def exchange(group, after):
            parts = slices(group)
            if after is not None:
                *parts, _ = lax.optimization_barrier((*parts, after))
            for d, part in zip(group, parts):
                g_parts[d] = send(part, d)

        exchange(G_GROUPS[0], None)

        own_inputs = [sinusoid(timesteps, freq_width), sinusoid(guidance, freq_width), pooled]
        outs = [mlp_forward(inputs_bf, params) for inputs_bf, params in zip(own_inputs, params_list)]
        cond_vec = outs[0] + outs[1] + outs[2]
        cond_silu = jax.nn.silu(cond_vec).astype(jnp.bfloat16)

        all_inputs = [sinusoid(times_all, freq_width), sinusoid(guides_all, freq_width), pooled_all]
        hidden_all, part_cond = embed_half(core, all_inputs, params_list, rows)
        outgoing = lax.dynamic_slice_in_dim(part_cond, (1 - core_id) * (batch // 2), batch // 2, axis=0)
        incoming = swap(outgoing)
        bias2 = (time_b2.astype(jnp.float32) + guide_b2.astype(jnp.float32) + text_b2.astype(jnp.float32))
        mine_t = sum_silu(core, part_cond, incoming, bias2[None])
        theirs_t = swap(mine_t)

        silu_their = swap(cond_silu)
        carry = None
        n_col = len(COLOURS)
        for call in CALLS:
            pick = []
            for r in call:
                for c, bits in enumerate(COLOURS):
                    pick.append((c, 0 if r == 0 else sum(bits[j] for j in ROUNDS[r - 1][0]) + bits[ROUNDS[r - 1][1]]))
            chips = [jnp.bitwise_xor(chip_id, d // 2) for _, d in pick]
            where = jnp.stack([(2 * q + core_id) * n_col + c for q, (c, _) in zip(chips, pick)] + chips + [jnp.int32(c) for c, _ in pick])
            carry = column_rounds(where, cond_silu, silu_their, d_mods, g_their, full_bmod, [held[c][d] for c, d in pick], carry)
        modulation, mod_their, d_parts = carry
        d_other = swap(d_parts[rows:])
        d_cond = d_parts[:rows] + d_other
        d_vec = d_cond * silu_grad(cond_vec)
        d_vec_bf = d_vec.astype(jnp.bfloat16)
        sums = jnp.sum(d_vec.reshape(16, rows // 16, hidden), axis=1)
        mod_mine = swap(mod_their)
        modulation = place_blocks(core, modulation, mod_mine)
        d_vec_all = lax.all_gather(d_vec_bf, MESH_AXIS, axis=0, tiled=True)
        sums_all = lax.all_gather(sums, MESH_AXIS, axis=0, tiled=True)
        grad_b2 = jnp.sum(sums_all, axis=0)
        exchange(G_GROUPS[1], d_vec_all)
        exchange(G_GROUPS[2], d_vec_all)

        grads = {}
        for which in ((2,), (0, 1)):
            mine = embed_grad(core, d_vec_all, which, all_inputs, hidden_all, params_list, rows)
            for pos, k in enumerate(which):
                whole = []
                for value, axis in zip(mine[3 * pos:3 * pos + 3], (1, 1, 0)):
                    whole.append(join_halves(core, value, swap(value), axis))
                grads[k] = (whole[0], whole[1][0], whole[2], grad_b2)

        g_parts[1] = lax.dynamic_index_in_dim(g_their, chip_id, 0, keepdims=False)
        totals = None
        for group in ((0, 1) + G_GROUPS[0], G_GROUPS[1], G_GROUPS[2]):
            peers = [jnp.bitwise_xor(me, d) for d in group]
            where = jnp.stack([p % (n_dev // 2) for p in peers] + [(p // (n_dev // 2) == core_id).astype(jnp.int32) for p in peers] + [me])
            totals = mod_weight_grad(where, mine_t, theirs_t, [(d_mods, True) if d == 0 else (g_parts[d], False) for d in group], cols, totals)
        return (modulation, totals[0], totals[1][0]) + grads[0] + grads[1] + grads[2]


    return jax.shard_map(local_step, mesh=mesh, in_specs=in_specs, out_specs=out_specs, check_vma=False)
```
